32 devices in a mesh: batch: 4 (over y, core), tensor: 2 (over x), latent: 4 (over z).
Axes of the slice: x: 2, y: 2, z: 4, core: 2. Of those that a mesh axis runs over, the one named last changes fastest.
Arguments:
- residual: bfloat16 [1024, 3584], P('batch', ('tensor', 'latent')), may hold values from -6 to 6
- target: bfloat16 [1024, 3584], P('batch', ('tensor', 'latent')), may hold values from -6 to 6
- encoder_weight: bfloat16 [3584, 32768], P(None, ('tensor', 'latent')), may hold values from -0.09375 to 0.09375
- encoder_bias: bfloat16 [32768], P(('tensor', 'latent')), may hold values from -0.59765625 to 0.29882812
- decoder_weight: bfloat16 [32768, 3584], P(('tensor', 'latent')), may hold values from -0.0625 to 0.0625
- decoder_bias: bfloat16 [3584], replicated, may hold values from -3 to 3
- first_gain: bfloat16 [3584], replicated, may hold values from 0.5 to 1.5
- second_gain: bfloat16 [3584], replicated, may hold values from 0.5 to 1.5
- gate_weight: bfloat16 [3584, 7168], P(None, ('tensor', 'latent')), may hold values from -0.09375 to 0.09375
- up_weight: bfloat16 [3584, 7168], P(None, ('tensor', 'latent')), may hold values from -0.09375 to 0.09375
- down_weight: bfloat16 [7168, 3584], P(('tensor', 'latent')), may hold values from -0.09375 to 0.09375
Outputs:
- encoder_grad: bfloat16 [3584, 32768], P('batch', ('tensor', 'latent'))
- decoder_grad: bfloat16 [32768, 3584], P(('tensor', 'latent'), 'batch')
The draws below stay inside these ranges and needn't reach their ends.
All inputs are finite; a program needn't handle non-finite values.
Results may differ from the reference program's by a relative error of at most 0.012.
The reference program's roundings to bfloat16 on the way (of `centered`, `latents`, `normed_input`, `hidden`, `grad_output`, `grad_recon` and `grad_preact`) count: a program that leaves them out, or rounds other values in their place, can miss the bound.
Values may be sent and summed in bfloat16 or wider, within the bound.
A program may use at most 192 MiB of HBM per device.

```python
import jax
import jax.numpy as jnp
from jax import lax

D = 3584
FF = 7168
LAT = 32768
TOKENS = 1024


def raised(values, own_key, source, target, parts, factor):
    def block_of(axis_at):
        return (jnp.arange(values.shape[axis_at]) // (values.shape[axis_at] // parts)).reshape((-1,) + (1,) * (values.ndim - 1 - axis_at))

    first = jax.random.permutation(own_key, parts)[block_of(target)]
    far = (block_of(target) + parts // 2) % parts
    return jnp.where((block_of(source) == first) | (block_of(source) == far), factor * values, values)


def shard_levels(key, extent, split, smallest, top_value):
    level = 1.0
    for dim, parts in split:
        heights = jax.random.uniform(jax.random.fold_in(jax.random.fold_in(key, 6), dim), (parts,), jnp.float32, smallest / len(split), top_value / len(split))
        level = level * jnp.repeat(jnp.exp(heights), extent[dim] // parts).reshape((-1,) + (1,) * (len(extent) - 1 - dim))
    return level


def scatter_about(rng, extent, width, reach, cuts=(), dtype=jnp.bfloat16):
    values = width * jax.random.normal(rng, extent, jnp.float32)
    if cuts:
        values = values * shard_levels(rng, extent, cuts, -0.22, 0.18)
    return jnp.clip(values, -reach, reach).astype(dtype)


def gaussian_with(rng, shape, scale, reach, shards, heavy, kind=jnp.bfloat16):
    array = scale * jax.random.normal(rng, shape, jnp.float32)
    if shards:
        array = array * shard_levels(rng, shape, shards, -0.22, 0.18)
    return jnp.clip(raised(array, jax.random.fold_in(rng, 3), *heavy), -reach, reach).astype(kind)


def setup_inputs(seed: int = 0) -> dict:
    key_of = jax.random.split(jax.random.key(seed), 12)
    residual = scatter_about(key_of[0], (TOKENS, D), 1.0, 6.0, ((0, 4), (1, 8)))
    target = scatter_about(key_of[1], (TOKENS, D), 1.0, 6.0, ((0, 4), (1, 8)))
    encoder_weight = scatter_about(key_of[2], (D, LAT), D ** -0.5, 0.09375, ((1, 8),))
    encoder_bias = jnp.clip(-0.59765625 + 0.8964844 * jax.random.uniform(key_of[3], (LAT,), jnp.float32) ** shard_levels(key_of[3], (LAT,), ((0, 8),), -0.2, 0.2), -0.59765625, 0.29882812).astype(jnp.bfloat16)
    decoder_weight = gaussian_with(key_of[4], (LAT, D), (LAT // 2) ** -0.5, 0.0625, ((0, 8),), (0, 1, 8, 2.0))
    decoder_bias = scatter_about(key_of[5], (D,), 0.5, 3.0)
    first_gain = jnp.clip(1.0 + 0.1 * jax.random.normal(key_of[6], (D,), jnp.float32), 0.5, 1.5).astype(jnp.bfloat16)
    second_gain = jnp.clip(1.0 + 0.1 * jax.random.normal(key_of[7], (D,), jnp.float32), 0.5, 1.5).astype(jnp.bfloat16)
    gate_weight = scatter_about(key_of[8], (D, FF), D ** -0.5, 0.09375, ((1, 8),))
    up_weight = scatter_about(key_of[9], (D, FF), D ** -0.5, 0.09375, ((1, 8),))
    down_weight = gaussian_with(key_of[10], (FF, D), FF ** -0.5, 0.09375, ((0, 8),), (0, 1, 8, 2.0))
    return dict(residual=residual, target=target, encoder_weight=encoder_weight, encoder_bias=encoder_bias, decoder_weight=decoder_weight, decoder_bias=decoder_bias, first_gain=first_gain, second_gain=second_gain, gate_weight=gate_weight, up_weight=up_weight, down_weight=down_weight)


epsilon = 1e-06

def reference(residual, target, encoder_weight, encoder_bias, decoder_weight, decoder_bias, first_gain, second_gain, gate_weight, up_weight, down_weight):
    f32 = jnp.float32
    bf16 = jnp.bfloat16
    contract_last = (((1,), (1,)), ((), ()))
    centered = (residual.astype(f32) - decoder_bias.astype(f32)).astype(bf16)
    preact = jnp.dot(centered, encoder_weight, preferred_element_type=f32) + encoder_bias.astype(f32)
    latents = jnp.maximum(preact, 0.0).astype(bf16)
    recon = jnp.dot(latents, decoder_weight, preferred_element_type=f32) + decoder_bias.astype(f32)
    scale_in = lax.rsqrt(lax.optimization_barrier(jnp.sum(recon * recon, axis=1, keepdims=True)) / D + epsilon)
    normed_input = (recon * scale_in * first_gain.astype(f32)).astype(bf16)
    gate_value = jnp.dot(normed_input, gate_weight, preferred_element_type=f32)
    up_value = jnp.dot(normed_input, up_weight, preferred_element_type=f32)
    gelu_value, gelu_back = jax.vjp(lambda v: jax.nn.gelu(v, approximate=True), gate_value)
    hidden = (gelu_value * up_value).astype(bf16)
    output = jnp.dot(hidden, down_weight, preferred_element_type=f32)
    scale_out = lax.rsqrt(lax.optimization_barrier(jnp.sum(output * output, axis=1, keepdims=True)) / D + epsilon)
    normed_out = output * scale_out
    result = recon + normed_out * second_gain.astype(f32)
    grad_result = 2.0 * (result - target.astype(f32)) / TOKENS
    grad_normed = grad_result * second_gain.astype(f32)
    inner_out = lax.optimization_barrier(jnp.sum(grad_normed * normed_out, axis=1, keepdims=True)) / D
    grad_output = (scale_out * (grad_normed - normed_out * inner_out)).astype(bf16)
    grad_hidden = lax.dot_general(grad_output, down_weight, contract_last, preferred_element_type=f32)
    grad_gate = gelu_back(grad_hidden * up_value)[0].astype(bf16)
    grad_up = (grad_hidden * gelu_value).astype(bf16)
    grad_normed_in = lax.dot_general(grad_gate, gate_weight, contract_last, preferred_element_type=f32)
    grad_normed_in = grad_normed_in + lax.dot_general(grad_up, up_weight, contract_last, preferred_element_type=f32)
    unit = recon * scale_in
    grad_unit = grad_normed_in * first_gain.astype(f32)
    inner_in = lax.optimization_barrier(jnp.sum(grad_unit * unit, axis=1, keepdims=True)) / D
    grad_recon = (grad_result + scale_in * (grad_unit - unit * inner_in)).astype(bf16)
    grad_latent = lax.dot_general(grad_recon, decoder_weight, contract_last, preferred_element_type=f32)
    grad_preact = jnp.where(preact > 0, grad_latent, 0.0).astype(bf16)
    contract_first = (((0,), (0,)), ((), ()))
    decoder_grad = lax.dot_general(latents, grad_recon, contract_first, preferred_element_type=f32)
    encoder_grad = lax.dot_general(centered, grad_preact, contract_first, preferred_element_type=f32)
    return (encoder_grad.astype(bf16), decoder_grad.astype(bf16))
```

```python
import functools

import jax
import jax.numpy as jnp
from jax import lax
from jax.experimental import pallas as pl
from jax.experimental.pallas import tpu as pltpu
from jax.sharding import PartitionSpec as P

epsilon = 1e-06
MESH = pl.DeviceIdType.MESH
f32 = jnp.float32
bf16 = jnp.bfloat16


def far_first(n):
    return sorted(range(1, n), key=lambda e: -min(e, n - e))


def remote(src, dst, send, recv, **where):
    return pltpu.make_async_remote_copy(
        src_ref=src, dst_ref=dst, send_sem=send, recv_sem=recv, device_id=where, device_id_type=MESH
    )


def place(nt, nz):
    t, z = lax.axis_index("tensor"), lax.axis_index("latent")
    return t, z, lambda d: lax.rem(t + d, nt), lambda e: lax.rem(z + e, nz)


def meet(peers):
    barrier = pltpu.get_barrier_semaphore()
    for where in peers:
        pl.semaphore_signal(barrier, inc=1, device_id=where, device_id_type=MESH)
    pl.semaphore_wait(barrier, len(peers))


def gather_copies(nt, nz, part, lat_send, lat_recv, ten_send, ten_recv):
    t, z, tt, zz = place(nt, nz)
    sends = []
    own = part(t, z)
    for e in far_first(nz):
        c = remote(own, own, lat_send.at[e], lat_recv.at[e], latent=zz(e))
        c.start()
        sends.append(c)
    for d in range(1, nt):
        c = remote(own, own, ten_send.at[d, 0], ten_recv.at[d, 0], tensor=tt(d))
        c.start()
        sends.append(c)
    for e in reversed(far_first(nz)):
        came = part(t, zz(nz - e))
        remote(came, came, lat_send.at[e], lat_recv.at[e], latent=zz(e)).wait_recv()
        for d in range(1, nt):
            c = remote(came, came, ten_send.at[d, e], ten_recv.at[d, e], tensor=tt(d))
            c.start()
            sends.append(c)
    for d in range(1, nt):
        for e in range(nz):
            came = part(tt(nt - d), zz(nz - e))
            remote(came, came, ten_send.at[d, e], ten_recv.at[d, e], tensor=tt(d)).wait_recv()
    for c in sends:
        c.wait_send()


def first_kernel(
    nt, nz, centered_ref, target_ref, out_ref, rows_ref,
    lat_send, lat_recv, ten_send, ten_recv, row_send, row_recv,
):
    t, z, tt, zz = place(nt, nz)
    rows = target_ref.shape[0] // (nt * nz)
    others = [(d, e) for d in range(nt) for e in range(nz) if d or e]
    me = t * nz + z
    out_ref[me] = centered_ref[...]
    mine = pl.ds(pl.multiple_of(me * rows, rows), rows)
    rows_ref[me] = target_ref[mine]
    meet([{"tensor": tt(d), "latent": zz(e)} for d, e in others])
    copies = []
    for d, e in others:
        there = pl.ds(pl.multiple_of((tt(d) * nz + zz(e)) * rows, rows), rows)
        c = remote(
            target_ref.at[there], rows_ref.at[me], row_send.at[d, e], row_recv.at[d, e],
            tensor=tt(d), latent=zz(e),
        )
        c.start()
        copies.append(c)
    gather_copies(
        nt, nz, lambda a, b: out_ref.at[a * nz + b], lat_send, lat_recv, ten_send, ten_recv
    )
    for (d, e), c in zip(others, copies):
        c.wait_send()
        slot = rows_ref.at[tt(nt - d) * nz + zz(nz - e)]
        remote(
            slot, slot, row_send.at[d, e], row_recv.at[d, e], tensor=tt(d), latent=zz(e)
        ).wait_recv()


def exchange_kernel(nt, nz, inputs, outputs, row_math, partial_ref, *refs):
    ins = refs[:inputs]
    out_ref = refs[inputs]
    outs = refs[inputs + 1 : inputs + 1 + outputs]
    (
        ten_buf, sum_buf, lat_buf, xs, xr, ys, yr, lat_send, lat_recv, ten_send, ten_recv,
    ) = refs[inputs + 1 + outputs :]
    t, z, tt, zz = place(nt, nz)
    rows = partial_ref.shape[0] // (nt * nz)

    def part_rows(a, b):
        return pl.ds(pl.multiple_of((a * nz + b) * rows, rows), rows)

    meet(
        [{"tensor": tt(d)} for d in range(1, nt)] + [{"latent": zz(e)} for e in range(1, nz)]
    )
    order = far_first(nz) + [0]
    sends = []
    firsts = {}
    for e in order:
        for d in range(1, nt):
            c = remote(
                partial_ref.at[part_rows(tt(d), zz(e))], ten_buf.at[d - 1, e],
                xs.at[d, e], xr.at[d, e], tensor=tt(d),
            )
            c.start()
            firsts[d, e] = c
    total = None
    for e in order:
        total = partial_ref[part_rows(t, zz(e))].astype(f32)
        for d in range(1, nt):
            firsts[d, e].wait()
            total = total + ten_buf[d - 1, e].astype(f32)
        if e:
            sum_buf[e - 1] = total.astype(bf16)
            c = remote(
                sum_buf.at[e - 1], lat_buf.at[e - 1], ys.at[e], yr.at[e], latent=zz(e)
            )
            c.start()
            sends.append(c)
    for c in sends:
        c.wait()
    for e in range(1, nz):
        total = total + lat_buf[e - 1].astype(f32)
    row_math(total, ins, outs, lambda value: out_ref.__setitem__(part_rows(t, z), value))
    gather_copies(
        nt, nz, lambda a, b: out_ref.at[part_rows(a, b)], lat_send, lat_recv, ten_send, ten_recv
    )


def mean_square_scale(rows):
    return lax.rsqrt(jnp.mean(rows * rows, axis=1, keepdims=True) + epsilon)


def recon_math(total, ins, outs, put):
    bias, gain = ins
    recon = total + bias[...].astype(f32)
    outs[0][...] = recon
    put((recon * mean_square_scale(recon) * gain[...].astype(f32)).astype(bf16))


def output_math(token_count, total, ins, outs, put):
    recon, target, gain_ref = ins
    gain = gain_ref[...].astype(f32)
    scale_out = mean_square_scale(total)
    normed_out = total * scale_out
    result = recon[...] + normed_out * gain
    grad_result = (2.0 / token_count) * (result - target[...].astype(f32))
    outs[0][...] = grad_result
    grad_normed = grad_result * gain
    inner = jnp.mean(grad_normed * normed_out, axis=1, keepdims=True)
    put((scale_out * (grad_normed - normed_out * inner)).astype(bf16))


def input_math(total, ins, outs, put):
    recon_ref, grad_result, gain = ins
    recon = recon_ref[...]
    scale_in = mean_square_scale(recon)
    unit = recon * scale_in
    grad_unit = total * gain[...].astype(f32)
    inner = jnp.mean(grad_unit * unit, axis=1, keepdims=True)
    put((grad_result[...] + scale_in * (grad_unit - unit * inner)).astype(bf16))


VMEM = pl.BlockSpec(memory_space=pltpu.VMEM)
DMA = pltpu.SemaphoreType.DMA


def priced(byte_count):
    return pl.CostEstimate(flops=0, bytes_accessed=byte_count, transcendentals=0)


def exchange(nt, nz, ident, row_math, partial, ins, row_outputs):
    tokens, width = partial.shape
    rows = tokens // (nt * nz)
    shape = jax.ShapeDtypeStruct
    return pl.pallas_call(
        functools.partial(exchange_kernel, nt, nz, len(ins), row_outputs, row_math),
        out_shape=[shape((tokens, width), bf16)] + [shape((rows, width), f32)] * row_outputs,
        in_specs=[VMEM] * (1 + len(ins)),
        out_specs=[VMEM] * (1 + row_outputs),
        scratch_shapes=[
            pltpu.VMEM((max(nt - 1, 1), nz, rows, width), bf16),
            pltpu.VMEM((max(nz - 1, 1), rows, width), bf16),
            pltpu.VMEM((max(nz - 1, 1), rows, width), bf16),
            DMA((nt, nz)), DMA((nt, nz)), DMA((nz,)), DMA((nz,)),
            DMA((nz,)), DMA((nz,)), DMA((nt, nz)), DMA((nt, nz)),
        ],
        compiler_params=pltpu.CompilerParams(collective_id=ident, has_side_effects=True),
        cost_estimate=priced(100_000_000),
        name=f"exchange_{ident}",
    )(partial, *ins)


def swap(x, k):
    n = lax.axis_size("batch")
    return lax.ppermute(x, "batch", [(i, i ^ k) for i in range(n)])


def spread(x):
    pieces = [x]
    for k in range(1, lax.axis_size("batch")):
        pieces.append(swap(pieces[k - 1], 1) if k > 1 and k % 2 else swap(x, k))
    return pieces


def blocks(x):
    n = lax.axis_size("batch")
    b = lax.axis_index("batch")
    width = x.shape[1] // n
    return [
        swap(part, k) if k else part
        for k in range(n)
        for part in [lax.dynamic_slice_in_dim(x, (b ^ k) * width, width, 1)]
    ]


def per_device(
    residual, target, encoder_weight, encoder_bias, decoder_weight, decoder_bias,
    first_gain, second_gain, gate_weight, up_weight, down_weight,
):
    contract_last = (((1,), (1,)), ((), ()))
    contract_first = (((0,), (0,)), ((), ()))
    nt, nz = lax.axis_size("tensor"), lax.axis_size("latent")
    n = nt * nz
    tokens, share = residual.shape
    width = share * n
    rows = tokens // n
    token_count = tokens * lax.axis_size("batch")
    offset = lax.axis_index(("tensor", "latent")) * share
    bias_share = lax.dynamic_slice_in_dim(decoder_bias.astype(f32), offset, share)
    centered_share = (residual.astype(f32) - bias_share).astype(bf16)
    shape = jax.ShapeDtypeStruct
    gathered, target_parts = pl.pallas_call(
        functools.partial(first_kernel, nt, nz),
        out_shape=[shape((n, tokens, share), bf16), shape((n, rows, share), bf16)],
        in_specs=[VMEM] * 2,
        out_specs=[VMEM] * 2,
        scratch_shapes=[
            DMA((nz,)), DMA((nz,)), DMA((nt, nz)), DMA((nt, nz)), DMA((nt, nz)), DMA((nt, nz)),
        ],
        compiler_params=pltpu.CompilerParams(collective_id=0, has_side_effects=True),
        cost_estimate=priced(60_000_000),
        name="exchange_0",
    )(centered_share, target)
    centered = gathered.transpose(1, 0, 2).reshape(tokens, width)
    target_rows = target_parts.transpose(1, 0, 2).reshape(rows, width)

    preact = jnp.dot(centered, encoder_weight, preferred_element_type=f32)
    latents = jnp.maximum(preact + encoder_bias.astype(f32), 0.0).astype(bf16)
    latent_pieces = spread(latents)
    centered_pieces = blocks(centered)
    partial_recon = jnp.dot(latents, decoder_weight, preferred_element_type=f32).astype(bf16)
    bias, gain_in, gain_out = (v.reshape(1, width) for v in (decoder_bias, first_gain, second_gain))
    normed_input, recon = exchange(nt, nz, 1, recon_math, partial_recon, (bias, gain_in), 1)
    gate_value = jnp.dot(normed_input, gate_weight, preferred_element_type=f32)
    up_value = jnp.dot(normed_input, up_weight, preferred_element_type=f32)
    gelu_value, gelu_back = jax.vjp(lambda v: jax.nn.gelu(v, approximate=True), gate_value)
    hidden = (gelu_value * up_value).astype(bf16)
    partial_out = jnp.dot(hidden, down_weight, preferred_element_type=f32).astype(bf16)
    grad_output, grad_result = exchange(
        nt, nz, 2, functools.partial(output_math, token_count), partial_out,
        (recon, target_rows, gain_out), 1,
    )
    grad_hidden = lax.dot_general(
        grad_output, down_weight, contract_last, preferred_element_type=f32
    )
    grad_gate = gelu_back(grad_hidden * up_value)[0].astype(bf16)
    grad_up = (grad_hidden * gelu_value).astype(bf16)
    partial_input = lax.dot_general(
        grad_gate, gate_weight, contract_last, preferred_element_type=f32
    )
    partial_input = partial_input + lax.dot_general(
        grad_up, up_weight, contract_last, preferred_element_type=f32
    )
    partial_input, latent_pieces, centered_pieces = lax.optimization_barrier(
        (partial_input.astype(bf16), latent_pieces, centered_pieces)
    )
    latents_all = jnp.concatenate(latent_pieces, axis=0)
    centered_block = jnp.concatenate(centered_pieces, axis=0)
    (grad_recon,) = exchange(
        nt, nz, 3, input_math, partial_input, (recon, grad_result, gain_in), 0
    )
    chunks = 4
    step = latents.shape[1] // chunks
    spread_chunks = []
    for c in range(chunks):
        grad_latent = lax.dot_general(
            grad_recon, decoder_weight[c * step : (c + 1) * step], contract_last,
            preferred_element_type=f32,
        )
        mask = latents[:, c * step : (c + 1) * step] > 0
        spread_chunks.append(spread(jnp.where(mask, grad_latent, 0.0).astype(bf16)))
    recon_block = jnp.concatenate(blocks(grad_recon), axis=0)
    decoder_grad = lax.dot_general(
        latents_all, recon_block, contract_first, preferred_element_type=f32
    ).astype(bf16)
    encoder_grad = jnp.concatenate(
        [
            lax.dot_general(
                centered_block, jnp.concatenate(pieces, axis=0), contract_first,
                preferred_element_type=f32,
            ).astype(bf16)
            for pieces in spread_chunks
        ],
        axis=1,
    )
    return (encoder_grad, decoder_grad)


def solution(mesh):
    in_specs = (
        P("batch", ("tensor", "latent")),
        P("batch", ("tensor", "latent")),
        P(None, ("tensor", "latent")),
        P(("tensor", "latent")),
        P(("tensor", "latent"), None),
        P(),
        P(),
        P(),
        P(None, ("tensor", "latent")),
        P(None, ("tensor", "latent")),
        P(("tensor", "latent"), None),
    )
    out_specs = (P("batch", ("tensor", "latent")), P(("tensor", "latent"), "batch"))
    return jax.shard_map(
        per_device, mesh=mesh, in_specs=in_specs, out_specs=out_specs, check_vma=False
    )
```
